32 devices in a mesh: groups: 2 (over y), seq: 8 (over z, core), heads: 2 (over x), sub: 1.
Axes of the slice: x: 2, y: 2, z: 4, core: 2. Of those that a mesh axis runs over, the one named last changes fastest.
Arguments:
- video_q: bfloat16 [5120, 2048], P(('groups', 'seq'), ('heads', 'sub')), parts along dimension 0, may hold values from -10 to 10
- video_cross_keys: bfloat16 [5120, 2048], P(('groups', 'seq'), ('heads', 'sub')), parts along dimension 0, may hold values from -10 to 10
- video_v: bfloat16 [5120, 2048], P(('groups', 'seq'), ('heads', 'sub')), parts along dimension 0, may hold values from -6 to 6
- audio_q: bfloat16 [1280, 2048], P(('groups', 'seq'), ('heads', 'sub')), parts along dimension 0, may hold values from -10 to 10
- audio_k: bfloat16 [1280, 2048], P(('groups', 'seq'), ('heads', 'sub')), parts along dimension 0, may hold values from -10 to 10
- audio_v: bfloat16 [1280, 2048], P(('groups', 'seq'), ('heads', 'sub')), parts along dimension 0, may hold values from -6 to 6
- audio_self_q: bfloat16 [1280, 2048], P(('groups', 'seq'), ('heads', 'sub')), parts along dimension 0, may hold values from -10 to 10
- audio_self_keys: bfloat16 [1280, 2048], P(('groups', 'seq'), ('heads', 'sub')), parts along dimension 0, may hold values from -10 to 10
- audio_self_v: bfloat16 [1280, 2048], P(('groups', 'seq'), ('heads', 'sub')), parts along dimension 0, may hold values from -6 to 6
- video_counts: int32 [16], P('groups'), parts along dimension 0, may hold values from 1 to 320, 2048 in all
- audio_counts: int32 [16], P('groups'), parts along dimension 0, may hold values from 1 to 80, 512 in all
- window_start: int32 [16], P('groups'), parts along dimension 0, may hold values from 0 to 3, as said below
- window_end: int32 [16], P('groups'), parts along dimension 0, may hold values from 1 to 4, as said below
Outputs:
- video_out: bfloat16 [5120, 2048], P(('groups', 'seq'), ('heads', 'sub')), parts along dimension 0
- audio_out: bfloat16 [1280, 2048], P(('groups', 'seq'), ('heads', 'sub')), parts along dimension 0
The draws below stay inside these ranges and needn't reach their ends.
There are 2 independent parts, one for each index of `groups`. The reference program is written for one: setup_inputs(seed, part) draws one part's arguments, and reference() takes and returns one part's arrays. A program takes and returns all parts, laid end to end along the dimension named above; each array names one. Nothing has to cross between parts.
Inputs may be any that keep to these rules, and one draw needn't show every extreme that they name: `video_counts`: the live tokens of each seq index's block of slots come first in it. `audio_counts`: the live tokens of each seq index's block of slots come first in it. window_start[f] is f // 2 or one less, never below 0, except for the frames with f // 2 = 2, whose window holds all 4 blocks. window_end[f] is f // 2 plus one or two, never above 4, except for the frames whose window holds all blocks.
All inputs are finite; a program needn't handle non-finite values.
Results may differ from the reference program's by a relative error of at most 0.0085.
Values may be sent and summed in bfloat16 or wider, within the bound.
No kernel may reach another device: no remote copies, remote signals or barrier semaphores. Data moves between devices by JAX's collectives and lax.ppermute only.
A program may use at most 64 MiB of HBM per device.

```python
import math
import jax
import jax.numpy as jnp
import numpy as np
from jax import lax

HEADS = 32
HD = 64
FRAME_TOKENS = 256
AUDIO_WIN_BLOCK = 128
VCAP = 320
ACAP = 80
VTOK = 2048
LIVE_AUDIO_TOKEN = 512
VSLOTS = 2560
ASLOTS = 640
NF = 8
NAB = 4
N_SEQ = 8


def drawn(key, tag, row_count, asking):
    columns = HEADS * HD
    spread = 2.5 if asking == 1 else 1.0
    values = jnp.clip(spread * jax.random.normal(jax.random.fold_in(key, tag * 10 + asking), (row_count, columns), jnp.float32), -10.0, 10.0)
    return values.astype(jnp.bfloat16)


def draw_video_q(key, part):
    return drawn(key, 1, VSLOTS, 1)


def draw_audio_k(key, part):
    return drawn(key, 1, ASLOTS, 0)


def draw_audio_q(key, part):
    return drawn(key, 2, ASLOTS, 1)


def draw_video_cross_keys(key, part):
    return drawn(key, 2, VSLOTS, 0)


def draw_audio_self_q(key, part):
    return drawn(key, 3, ASLOTS, 1)


def draw_audio_self_keys(key, part):
    return drawn(key, 3, ASLOTS, 0)


def frame_windows(key):
    ratio = NF // NAB
    frames = jnp.arange(NF, dtype=jnp.int32)
    center = frames // ratio
    below = jax.random.randint(jax.random.fold_in(key, 71), (NF,), 0, 2, dtype=jnp.int32)
    above = jax.random.randint(jax.random.fold_in(key, 72), (NF,), 0, 2, dtype=jnp.int32)
    forced = frames == (NAB // 2 - 1) * ratio
    below = jnp.where(forced, 1, below)
    above = jnp.where(forced, 1, above)
    wide = center == NAB // 2
    first = jnp.where(wide, 0, jnp.maximum(center - below, 0)).astype(jnp.int32)
    final = jnp.where(wide, NAB, jnp.minimum(center + 1 + above, NAB)).astype(jnp.int32)
    return (first, final)


def draw_window_start(key, part):
    return frame_windows(key)[0]


def draw_window_end(key, part):
    return frame_windows(key)[1]


def level_of(own_key, shape, shards, smallest, largest):
    loudness, own = 1.0, jax.random.fold_in(own_key, 6)
    for dim, shards_of in shards:
        heights = jnp.exp(jax.random.uniform(jax.random.fold_in(own, dim), (shards_of,), jnp.float32, smallest / len(shards), largest / len(shards)))
        loudness = loudness * jnp.repeat(heights, shape[dim] // shards_of).reshape([-1 if axis == dim else 1 for axis in range(len(shape))])
    return loudness


def profile(count, total, most, lean):
    loads = [(1 << 20) // math.isqrt(standing ** lean) + 1 for standing in range(2, count + 1)]
    rest, given = total - most - (count - 1), [1] * (count - 1)
    while rest > 0:
        free = [i for i in range(count - 1) if given[i] < most]
        whole, budget = sum([loads[i] for i in free]), rest
        for i in free:
            addition = min(most - given[i], max(1, budget * loads[i] // whole), rest)
            given[i] = given[i] + addition
            rest = rest - addition
    return np.array([most] + given)


def ragged_sizes(key, number_of, total, bound, skew):
    if number_of == 2:
        one = jax.random.randint(key, (), max(1, total - bound), min(bound, total - 1) + 1)
        return jnp.stack([one, total - one])
    tallies = jnp.asarray(profile(number_of, total, bound, skew), jnp.int32)
    couples = (number_of - 1) // 2
    source_of, sink = tallies[1:1 + 2 * couples:2], tallies[2:2 + 2 * couples:2]
    margin = jnp.minimum(source_of - 1, bound - sink)
    shifted = jax.random.randint(jax.random.fold_in(key, 1), (couples,), 0, 1 << 20) % (margin + 1)
    tallies = tallies.at[1:1 + 2 * couples:2].set(source_of - shifted).at[2:2 + 2 * couples:2].set(sink + shifted)
    return tallies[jax.random.permutation(jax.random.fold_in(key, 2), number_of)]


def scatter_about(stream_key, dims, width, most, shards=(), kind=jnp.bfloat16):
    loudness = level_of(stream_key, dims, shards, -0.22, 0.18) if shards else 1.0
    result = jax.random.normal(stream_key, dims, jnp.float32) * width * loudness
    return jnp.minimum(jnp.maximum(result, -most), most).astype(kind)


def setup_inputs(seed: int = 0, part: int = 0) -> dict:
    splits = jax.random.split(jax.random.key(seed), 14)
    own_keys = jax.random.split(jax.random.fold_in(splits[13], part), 14)
    video_q = draw_video_q(jax.random.fold_in(jax.random.fold_in(splits[13], part), 71), part)
    video_cross_keys = draw_video_cross_keys(jax.random.fold_in(jax.random.fold_in(splits[13], part), 71), part)
    video_v = scatter_about(own_keys[2], (VSLOTS, HEADS * HD), 1.0, 6.0, ((0, 8), (1, 2)))
    audio_q = draw_audio_q(jax.random.fold_in(jax.random.fold_in(splits[13], part), 71), part)
    audio_k = draw_audio_k(jax.random.fold_in(jax.random.fold_in(splits[13], part), 71), part)
    audio_v = scatter_about(own_keys[5], (ASLOTS, HEADS * HD), 1.0, 6.0, ((0, 8), (1, 2)))
    audio_self_q = draw_audio_self_q(jax.random.fold_in(jax.random.fold_in(splits[13], part), 71), part)
    audio_self_keys = draw_audio_self_keys(jax.random.fold_in(jax.random.fold_in(splits[13], part), 71), part)
    audio_self_v = scatter_about(own_keys[8], (ASLOTS, HEADS * HD), 1.0, 6.0, ((0, 8), (1, 2)))
    video_counts = ragged_sizes(own_keys[9], N_SEQ, VTOK, VCAP, 2).astype(jnp.int32)
    audio_counts = ragged_sizes(own_keys[10], N_SEQ, LIVE_AUDIO_TOKEN, ACAP, 2).astype(jnp.int32)
    window_start = draw_window_start(jax.random.fold_in(jax.random.fold_in(splits[13], part), 71), part)
    window_end = draw_window_end(jax.random.fold_in(jax.random.fold_in(splits[13], part), 71), part)
    return {"video_q": video_q, "video_cross_keys": video_cross_keys, "video_v": video_v, "audio_q": audio_q, "audio_k": audio_k, "audio_v": audio_v, "audio_self_q": audio_self_q, "audio_self_keys": audio_self_keys, "audio_self_v": audio_self_v, "video_counts": video_counts, "audio_counts": audio_counts, "window_start": window_start, "window_end": window_end}


NEG = -1e30


def slot_of(counts, capacity, total):
    ends = jnp.cumsum(counts).astype(jnp.int32)
    starts = (ends - counts).astype(jnp.int32)
    places = jnp.arange(total, dtype=jnp.int32)
    owner = jnp.sum((ends[None, :] <= places[:, None]).astype(jnp.int32), axis=1).astype(jnp.int32)
    return (owner * capacity + places - starts[owner]).astype(jnp.int32)


def attend_pairs(query, key_rows, values, allowed):
    scores = jnp.einsum("qhd,khd->qhk", query.astype(jnp.float32), key_rows.astype(jnp.float32)) * (HD ** -0.5)
    scores = jnp.where(allowed[:, None, :], scores, NEG)
    highest = jnp.max(scores, axis=2, keepdims=True)
    weights = jnp.where(allowed[:, None, :], jnp.exp(scores - highest), 0.0)
    total = jnp.sum(weights, axis=2)
    rounded = lax.optimization_barrier(weights.astype(jnp.bfloat16)).astype(jnp.float32)
    mixed = jnp.einsum("qhk,khd->qhd", rounded, values.astype(jnp.float32))
    return mixed / total[:, :, None]


def reference(video_q, video_cross_keys, video_v, audio_q, audio_k, audio_v, audio_self_q, audio_self_keys, audio_self_v, video_counts, audio_counts, window_start, window_end):
    def head_count(array, slots):
        return array[slots].reshape(slots.shape[0], HEADS, HD)

    video_slot_table = slot_of(video_counts, VCAP, VTOK)
    audio_slot_table = slot_of(audio_counts, ACAP, LIVE_AUDIO_TOKEN)
    vquery = head_count(video_q, video_slot_table)
    video_key_rows = head_count(video_cross_keys, video_slot_table)
    vvalues = head_count(video_v, video_slot_table)
    aquery = head_count(audio_q, audio_slot_table)
    akeys = head_count(audio_k, audio_slot_table)
    avalues = head_count(audio_v, audio_slot_table)
    squery = head_count(audio_self_q, audio_slot_table)
    self_key_rows = head_count(audio_self_keys, audio_slot_table)
    self_value_rows = head_count(audio_self_v, audio_slot_table)
    audio_block_of = (jnp.arange(LIVE_AUDIO_TOKEN, dtype=jnp.int32) // AUDIO_WIN_BLOCK).astype(jnp.int32)

    def video_frame(frame):
        row_count = lax.dynamic_slice_in_dim(vquery, (frame * FRAME_TOKENS).astype(jnp.int32), FRAME_TOKENS, 0)
        inside = (audio_block_of >= window_start[frame]) & (audio_block_of < window_end[frame])
        return attend_pairs(row_count, akeys, avalues, jnp.broadcast_to(inside[None, :], (FRAME_TOKENS, LIVE_AUDIO_TOKEN)))

    video_result = lax.map(video_frame, jnp.arange(NF, dtype=jnp.int32)).reshape(VTOK, HEADS * HD)

    frame_of = (jnp.arange(VTOK, dtype=jnp.int32) // FRAME_TOKENS).astype(jnp.int32)
    key_first = window_start[frame_of]
    key_final = window_end[frame_of]
    row_step = AUDIO_WIN_BLOCK // 4

    def audio_rows(index):
        first_row = (index * row_step).astype(jnp.int32)
        row_count = lax.dynamic_slice_in_dim(aquery, first_row, row_step, 0)
        block = first_row // AUDIO_WIN_BLOCK
        inside = (key_first <= block) & (block < key_final)
        return attend_pairs(row_count, video_key_rows, vvalues, jnp.broadcast_to(inside[None, :], (row_step, VTOK)))

    cross = lax.map(audio_rows, jnp.arange(LIVE_AUDIO_TOKEN // row_step, dtype=jnp.int32)).reshape(LIVE_AUDIO_TOKEN, HEADS, HD)
    united = (squery.astype(jnp.float32) + cross).astype(jnp.bfloat16)

    def self_block(block):
        row_count = lax.dynamic_slice_in_dim(united, (block * AUDIO_WIN_BLOCK).astype(jnp.int32), AUDIO_WIN_BLOCK, 0)
        return attend_pairs(row_count, self_key_rows, self_value_rows, jnp.ones((AUDIO_WIN_BLOCK, LIVE_AUDIO_TOKEN), dtype=bool))

    own = lax.map(self_block, jnp.arange(NAB, dtype=jnp.int32)).reshape(LIVE_AUDIO_TOKEN, HEADS, HD)
    audio_result = (cross + own).astype(jnp.bfloat16).reshape(LIVE_AUDIO_TOKEN, HEADS * HD)
    video_out = jnp.zeros((VSLOTS, HEADS * HD), jnp.bfloat16).at[video_slot_table].set(video_result.astype(jnp.bfloat16))
    audio_out = jnp.zeros((ASLOTS, HEADS * HD), jnp.bfloat16).at[audio_slot_table].set(audio_result)
    return video_out, audio_out
```

```python
import functools

import jax
import jax.numpy as jnp
from jax import lax
from jax.experimental import pallas as pl
from jax.experimental.pallas import tpu as pltpu
from jax.sharding import PartitionSpec as P

HD = 64
FRAME_TOKENS = 256
AUDIO_WIN_BLOCK = 128
LANES = 128
DEAD = LANES - 1
FAR = -1e30
FLOOR = -1e20
LOG2E = 1.4426950408889634
NT = (((1,), (1,)), ((), ()))
BF = jnp.bfloat16
F32 = jnp.float32


def lane_masks():
    low = lax.broadcasted_iota(jnp.int32, (1, LANES), 1) < HD
    low_f = jnp.where(low, 1.0, 0.0).astype(F32)
    return low, low_f.astype(BF), (1.0 - low_f).astype(BF)


def attend(q2, q_extra, keys, v2, masks):
    low, low_b, high_b = masks
    rows = q2.shape[0]
    both = jnp.concatenate(
        [
            jnp.concatenate([q2 * low_b, q_extra], axis=1),
            jnp.concatenate([q2 * high_b, q_extra], axis=1),
        ],
        axis=0,
    )
    s = lax.dot_general(both, keys, NT, preferred_element_type=F32)
    top = jnp.maximum(jnp.max(s, axis=1, keepdims=True), FLOOR)
    p = jnp.exp2((s - top) * (LOG2E * HD ** (-0.5)))
    total = jnp.sum(p, axis=1, keepdims=True)
    pb = p.astype(BF)
    mixed = jnp.dot(pb[:rows], v2 * low_b, preferred_element_type=F32) + jnp.dot(
        pb[rows:], v2 * high_b, preferred_element_type=F32
    )
    safe = jnp.where(total > 0, total, 1.0)
    inv = 1.0 / safe
    mixed = mixed * jnp.where(low, inv[:rows], inv[rows:])
    return mixed, top, safe


def pack_kernel(count, seat, *refs):
    for i in range(count):
        refs[count][i] = refs[i][...]


def tables_kernel(members, vslots, aslots, seat, vc, ac, ws, we, feat, bias):
    frames = ws.shape[0]
    lane = lax.broadcasted_iota(jnp.int32, (aslots, LANES), 1)
    row = lax.broadcasted_iota(jnp.int32, (aslots, LANES), 0)
    start = jnp.int32(0)
    for s in range(members):
        block = (row + start) // AUDIO_WIN_BLOCK
        hit = jnp.where(row < ac[s], block, DEAD) == lane
        feat[s * aslots : (s + 1) * aslots, :] = jnp.where(hit, 1.0, 0.0).astype(BF)
        start = start + ac[s]
    node = seat[0] // 2
    lane = lax.broadcasted_iota(jnp.int32, (vslots, LANES), 1)
    row = lax.broadcasted_iota(jnp.int32, (vslots, LANES), 0)
    for half in range(2):
        own = node * 2 + half
        start = lax.fori_loop(
            0, members, lambda s, t: t + jnp.where(s < own, vc[s], 0), jnp.int32(0)
        )
        frame = (row + start) // FRAME_TOKENS
        ok = lane < 0
        for f in range(frames):
            ok = ok | ((frame == f) & (lane >= ws[f]) & (lane < we[f]))
        ok = ok & (row < vc[own]) & (lane < DEAD)
        bias[half * vslots : (half + 1) * vslots, :] = jnp.where(ok, 0.0, FAR).astype(BF)


def chunk_kernel(aslots, seat, q, k, v, sk, sv, got, qc, kvc, sc):
    c = seat[0] % 2
    mine = pl.ds(pl.multiple_of(c * aslots, 16), aslots)
    other = pl.ds(pl.multiple_of((1 - c) * aslots, 16), aslots)
    qc[mine, :] = q[...]
    qc[other, :] = got[0]
    for i, (ref, out, slot) in enumerate(((k, kvc, 0), (v, kvc, 1), (sk, sc, 0), (sv, sc, 1))):
        out[slot, mine, :] = ref[...]
        out[slot, other, :] = got[1 + i]


def stat_block(st, heads, half):
    rest = st.T[:heads]
    parts = []
    for _ in range(3):
        part = rest.astype(BF).astype(F32)
        parts.append(part)
        rest = rest - part
    slabs = [p[:, j * LANES : (j + 1) * LANES] for p in parts for j in range(2)]
    slabs = slabs + [jnp.zeros_like(slabs[0])] * 2
    width = half // LANES
    groups = [
        jnp.concatenate(slabs[g : g + width], axis=1) if width > 1 else slabs[g]
        for g in range(0, 8, width)
    ]
    return jnp.concatenate(groups, axis=0).astype(BF)


def read_stats(block, heads, half, turn):
    width = half // LANES
    slabs = []
    for g in range(8 // width):
        rows = block[g * heads : (g + 1) * heads]
        for j in range(width):
            slabs.append(rows[:, j * LANES : (j + 1) * LANES])
    for j in range(2):
        turn[:heads, j * LANES : (j + 1) * LANES] = (slabs[j] + slabs[2 + j]) + slabs[4 + j]
    return turn[...].T


def audio_kernel(offsets, vslots, aslots, nodes, seat, feat, bias, ck, vv, got, *refs):
    count = len(offsets)
    chunks, outs = refs[:count], refs[count : 2 * count]
    kbuf, vbuf, stat = refs[2 * count :]
    half = kbuf.shape[1]
    pairs = half // LANES
    c = seat[0] % 2
    node = seat[0] // 2
    mine = pl.ds(pl.multiple_of(c * vslots, 16), vslots)
    other = pl.ds(pl.multiple_of((1 - c) * vslots, 16), vslots)
    kbuf[mine, :] = ck[...]
    kbuf[other, :] = got[1]
    vbuf[mine, :] = vv[...]
    vbuf[other, :] = got[2]
    masks = lane_masks()
    rows = 2 * aslots
    lane = lax.broadcasted_iota(jnp.int32, (rows, LANES), 1)
    stat[...] = jnp.zeros_like(stat)
    for offset, chunk, out in zip(offsets, chunks, outs):
        source = lax.rem(node + offset + nodes, nodes)
        extra = feat[pl.ds(pl.multiple_of(source * rows, 16), rows), :]

        @pl.loop(0, pairs)
        def _(p):
            cols = pl.ds(pl.multiple_of(p * LANES, LANES), LANES)
            keys = jnp.concatenate([kbuf[:, cols], bias[...]], axis=1)
            mixed, top, total = attend(chunk[:, cols], extra, keys, vbuf[:, cols], masks)
            out[:rows, cols] = mixed.astype(BF)
            lse = top * HD ** (-0.5) + jnp.log(total)
            st = stat[:rows, :]
            st = jnp.where(lane == 2 * p, lse[:rows], st)
            stat[:rows, :] = jnp.where(lane == 2 * p + 1, lse[rows:], st)

        out[rows:, :] = stat_block(stat[...], 2 * pairs, half)


def video_kernel(vslots, aslots, nodes, offsets, tile, seat, feat, bias, vq, got, *refs):
    chunks = refs[:nodes]
    own_out, other_out, kbuf, vbuf, fbuf = refs[nodes:]
    half = kbuf.shape[1]
    pairs = half // LANES
    c = seat[0] % 2
    node = seat[0] // 2
    rows = 2 * aslots
    for i, offset in enumerate(offsets):
        at = slice(i * rows, (i + 1) * rows)
        kbuf[at, :] = chunks[i][0]
        vbuf[at, :] = chunks[i][1]
        source = lax.rem(node + offset + nodes, nodes)
        fbuf[at, :] = feat[pl.ds(pl.multiple_of(source * rows, 16), rows), :]
    masks = lane_masks()
    for part in range(2):
        queries = vq if part == 0 else got.at[0]
        out = own_out if part == 0 else other_out
        base = (c if part == 0 else 1 - c) * vslots

        @pl.loop(0, pairs)
        def _(p):
            cols = pl.ds(pl.multiple_of(p * LANES, LANES), LANES)
            keys = jnp.concatenate([kbuf[:, cols], fbuf[...]], axis=1)
            v2 = vbuf[:, cols]
            for t in range(vslots // tile):
                at = slice(t * tile, (t + 1) * tile)
                extra = bias[pl.ds(pl.multiple_of(base + t * tile, 16), tile), :]
                mixed, _, _ = attend(queries[at, cols], extra, keys, v2, masks)
                out[at, cols] = mixed.astype(BF)


def self_kernel(aslots, nodes, offsets, seat, ac, feat, sq, got, *refs):
    partials = refs[:nodes]
    chunks = refs[nodes : 2 * nodes]
    own_out, other_out, kbuf, vbuf, fbuf, turn, qbuf, result = refs[2 * nodes :]
    half = kbuf.shape[1]
    pairs = half // LANES
    heads = 2 * pairs
    c = seat[0] % 2
    node = seat[0] // 2
    rows = 2 * aslots
    mine = pl.ds(pl.multiple_of(c * aslots, 16), aslots)
    other = pl.ds(pl.multiple_of((1 - c) * aslots, 16), aslots)
    qbuf[mine, :] = sq[...]
    qbuf[other, :] = got[5]
    for i, offset in enumerate(offsets):
        at = slice(i * rows, (i + 1) * rows)
        kbuf[at, :] = chunks[i][0]
        vbuf[at, :] = chunks[i][1]
        source = lax.rem(node + offset + nodes, nodes)
        fbuf[at, :] = feat[pl.ds(pl.multiple_of(source * rows, 16), rows), :]
    turn[...] = jnp.zeros_like(turn)
    stats = [
        read_stats(x[rows:, :].astype(F32), heads, half, turn)[:rows] for x in partials
    ]
    peak = functools.reduce(jnp.maximum, stats)
    weights = [jnp.exp(s - peak) for s in stats]
    inv = 1.0 / functools.reduce(jnp.add, weights)
    weights = [w * inv for w in weights]
    low, low_b, high_b = lane_masks()
    lane = lax.broadcasted_iota(jnp.int32, (rows, LANES), 1)
    row = lax.broadcasted_iota(jnp.int32, (rows, LANES), 0)
    bound = jnp.where(row < aslots, ac[2 * node], ac[2 * node + 1] + aslots)
    live = row < bound
    extra = jnp.where(lane == DEAD, FAR, 0.0).astype(BF)
    for p in range(pairs):
        cols = slice(p * LANES, (p + 1) * LANES)
        cross = jnp.zeros((rows, LANES), F32)
        for x, w in zip(partials, weights):
            share = jnp.where(low, w[:, 2 * p : 2 * p + 1], w[:, 2 * p + 1 : 2 * p + 2])
            cross = cross + x[:rows, cols].astype(F32) * share
        united = (qbuf[:, cols].astype(F32) + cross).astype(BF)
        keys = jnp.concatenate([kbuf[:, cols], fbuf[...]], axis=1)
        mixed, _, _ = attend(united, extra, keys, vbuf[:, cols], (low, low_b, high_b))
        result[:, cols] = jnp.where(live, cross + mixed, 0.0).astype(BF)
    own_out[...] = result[mine, :]
    other_out[...] = result[other, :]


def join_kernel(seat, own, got, out):
    half = own.shape[1]
    c = seat[0] % 2
    out[:, pl.ds(pl.multiple_of(c * half, LANES), half)] = own[...]
    out[:, pl.ds(pl.multiple_of((1 - c) * half, LANES), half)] = got[...]


def shards(
    video_q,
    video_cross_keys,
    video_v,
    audio_q,
    audio_k,
    audio_v,
    audio_self_q,
    audio_self_keys,
    audio_self_v,
    video_counts,
    audio_counts,
    window_start,
    window_end,
):
    seat = lax.axis_index("seq").astype(jnp.int32).reshape(1)
    members = lax.axis_size("seq")
    nodes = members // 2
    vslots, width = video_q.shape
    aslots = audio_q.shape[0]
    half = width // 2
    rows = 2 * aslots
    everyone = nodes * rows
    vmem = pl.BlockSpec(memory_space=pltpu.VMEM)
    smem = pl.BlockSpec(memory_space=pltpu.SMEM)
    sds = jax.ShapeDtypeStruct

    def own_half(slots):
        return pl.BlockSpec((slots, half), lambda i, s: (0, s[0] % 2))

    def other_half(slots):
        return pl.BlockSpec((slots, half), lambda i, s: (0, 1 - s[0] % 2))

    def full(*shape):
        return pl.BlockSpec(shape, lambda i, s: (0,) * len(shape))

    def call(body, ins, outs, args, scratch=(), flops=0, name=None):
        out_shapes, out_specs = outs
        moved = sum(x.size * x.dtype.itemsize for x in args)
        return pl.pallas_call(
            body,
            out_shape=out_shapes,
            grid_spec=pltpu.PrefetchScalarGridSpec(
                num_scalar_prefetch=1,
                grid=(1,),
                in_specs=ins,
                out_specs=out_specs,
                scratch_shapes=scratch,
            ),
            cost_estimate=pl.CostEstimate(
                flops=flops or moved, bytes_accessed=moved, transcendentals=0
            ),
            name=name,
        )(seat, *args)

    def outs(*shapes):
        return (
            [sds(s, BF) for s in shapes],
            [full(*s) for s in shapes],
        )

    def swap(x):
        return lax.ppermute(x, "seq", [(i, i ^ 1) for i in range(members)])

    def shift(x, by):
        return lax.ppermute(x, "seq", [(i, (i + 2 * by) % members) for i in range(members)])

    audio = (audio_q, audio_k, audio_v, audio_self_keys, audio_self_v, audio_self_q)
    (audio_send,) = call(
        functools.partial(pack_kernel, 6),
        [other_half(aslots)] * 6,
        outs((6, aslots, half)),
        audio,
        name="pack_audio",
    )
    audio_got = swap(audio_send)
    video = (video_q, video_cross_keys, video_v)
    (video_send,) = call(
        functools.partial(pack_kernel, 3),
        [other_half(vslots)] * 3,
        outs((3, vslots, half)),
        video,
        name="pack_video",
    )
    video_got = swap(video_send)
    feat, bias = call(
        functools.partial(tables_kernel, members, vslots, aslots),
        [smem] * 4,
        outs((everyone, LANES), (2 * vslots, LANES)),
        (video_counts, audio_counts, window_start, window_end),
        name="tables",
    )
    qc, kvc, sc = call(
        functools.partial(chunk_kernel, aslots),
        [own_half(aslots)] * 5 + [full(6, aslots, half)],
        outs((rows, half), (2, rows, half), (2, rows, half)),
        audio[:5] + (audio_got,),
        name="chunk",
    )

    def spread(x, turned):
        found = {}
        left = right = x
        for k in range(1, (nodes - 1) // 2 + 1):
            left, right = shift(left, 1), shift(right, -1)
            found[-k], found[k] = left, right
        if nodes % 2 == 0:
            found[nodes // 2] = shift(left, 1) if turned else shift(right, -1)
        return found

    q_of = spread(qc, False)
    kv_of = spread(kvc, True)
    s_of = spread(sc, False)

    unit = 4 * rows * 2 * vslots * LANES * 2

    def partial(offsets, chunks):
        payload = (rows + 16, half)
        return call(
            functools.partial(audio_kernel, offsets, vslots, aslots, nodes),
            [full(everyone, LANES), full(2 * vslots, LANES), own_half(vslots), own_half(vslots)]
            + [full(3, vslots, half)]
            + [full(rows, half)] * len(offsets),
            outs(*[payload] * len(offsets)),
            (feat, bias, video_cross_keys, video_v, video_got, *chunks),
            scratch=[
                pltpu.VMEM((2 * vslots, half), BF),
                pltpu.VMEM((2 * vslots, half), BF),
                pltpu.VMEM((2 * LANES, LANES), F32),
            ],
            flops=unit * len(offsets) * (half // LANES),
            name="audio",
        )

    parts = {}
    (parts[0],) = partial((0,), [qc])
    for k in range(1, (nodes - 1) // 2 + 1):
        to_left, to_right = partial((-k, k), [q_of[-k], q_of[k]])
        parts[k] = shift(to_left, -k)
        parts[-k] = shift(to_right, k)
    if nodes % 2 == 0:
        k = nodes // 2
        (far,) = partial((k,), [q_of[k]])
        parts[k] = shift(far, k)

    offsets = tuple(sorted(q_of))
    offsets = (0,) + offsets
    tile = 160 if vslots % 160 == 0 else vslots
    own_video, other_video = call(
        functools.partial(video_kernel, vslots, aslots, nodes, offsets, tile),
        [full(everyone, LANES), full(2 * vslots, LANES), own_half(vslots), full(3, vslots, half)]
        + [full(2, rows, half)] * nodes,
        outs((vslots, half), (vslots, half)),
        (feat, bias, video_q, video_got) + tuple(kvc if o == 0 else kv_of[o] for o in offsets),
        scratch=[
            pltpu.VMEM((everyone, half), BF),
            pltpu.VMEM((everyone, half), BF),
            pltpu.VMEM((everyone, LANES), BF),
        ],
        flops=unit * nodes * (half // LANES),
        name="video",
    )
    got_video = swap(other_video)

    def join(slots, own, got):
        return call(
            join_kernel,
            [full(slots, half)] * 2,
            outs((slots, width)),
            (own, got),
            name="join",
        )[0]

    video_out = join(vslots, own_video, got_video)
    own_audio, other_audio = call(
        functools.partial(self_kernel, aslots, nodes, offsets),
        [smem, full(everyone, LANES), own_half(aslots), full(6, aslots, half)]
        + [full(rows + 16, half)] * nodes
        + [full(2, rows, half)] * nodes,
        outs((aslots, half), (aslots, half)),
        (audio_counts, feat, audio_self_q, audio_got)
        + tuple(parts[o] for o in offsets)
        + tuple(sc if o == 0 else s_of[o] for o in offsets),
        scratch=[
            pltpu.VMEM((everyone, half), BF),
            pltpu.VMEM((everyone, half), BF),
            pltpu.VMEM((everyone, LANES), BF),
            pltpu.VMEM((LANES, 2 * LANES), F32),
            pltpu.VMEM((rows, half), BF),
            pltpu.VMEM((rows, half), BF),
        ],
        flops=unit * (half // LANES),
        name="self_attention",
    )
    audio_out = join(aslots, own_audio, swap(other_audio))
    return (video_out, audio_out)


def solution(mesh):
    split = P(("groups", "seq"), ("heads", "sub"))
    return jax.shard_map(
        shards,
        mesh=mesh,
        in_specs=(split,) * 9 + (P("groups"),) * 4,
        out_specs=(split, split),
        check_vma=False,
    )
```

```python
import functools

import jax
import jax.numpy as jnp
from jax import lax
from jax.experimental import pallas as pl
from jax.experimental.pallas import tpu as pltpu
from jax.sharding import PartitionSpec as P


HD = 64
FRAME_TOKENS = 256
AUDIO_WIN_BLOCK = 128
LANES = 128
DEAD = LANES - 1
FAR = -1e30
FLOOR = -1e20
LOG2E = 1.4426950408889634
NT = (((1,), (1,)), ((), ()))
BF = jnp.bfloat16
F32 = jnp.float32


def lane_masks():
    low = jnp.where(lax.broadcasted_iota(jnp.int32, (1, LANES), 1) < HD, 1.0, 0.0).astype(F32)
    return low.astype(BF), (1.0 - low).astype(BF)


def values_of(v2, masks):
    low, high = masks
    return (
        jnp.concatenate([v2 * low, jnp.broadcast_to(low, v2.shape)], axis=1),
        jnp.concatenate([v2 * high, jnp.broadcast_to(high, v2.shape)], axis=1),
    )


def attend(q2, q_extra, keys, values, masks):
    low, high = masks
    rows = q2.shape[0]
    both = jnp.concatenate(
        [
            jnp.concatenate([q2 * low, q_extra], axis=1),
            jnp.concatenate([q2 * high, q_extra], axis=1),
        ],
        axis=0,
    )
    s = lax.dot_general(both, keys, NT, preferred_element_type=F32)
    top = jnp.maximum(jnp.max(s, axis=1, keepdims=True), FLOOR)
    p = jnp.exp2((s - top) * (LOG2E * HD ** (-0.5))).astype(BF)
    mixed = jnp.dot(p[:rows], values[0], preferred_element_type=F32) + jnp.dot(
        p[rows:], values[1], preferred_element_type=F32
    )
    total = mixed[:, LANES:]
    total = jnp.where(total > 0, total, 1.0)
    return mixed[:, :LANES] / total, top, total


def pack_kernel(a, b, out):
    out[0] = a[...]
    out[1] = b[...]


def tables_kernel(members, vslots, aslots, seat, vc, ac, ws, we, feat, bias):
    frames = ws.shape[0]
    lane = lax.broadcasted_iota(jnp.int32, (aslots, LANES), 1)
    row = lax.broadcasted_iota(jnp.int32, (aslots, LANES), 0)
    start = jnp.int32(0)
    for s in range(members):
        block = (row + start) // AUDIO_WIN_BLOCK
        hit = jnp.where(row < ac[s], block, DEAD) == lane
        feat[s * aslots : (s + 1) * aslots, :] = jnp.where(hit, 1.0, 0.0).astype(BF)
        start = start + ac[s]
    lane = lax.broadcasted_iota(jnp.int32, (vslots, LANES), 1)
    row = lax.broadcasted_iota(jnp.int32, (vslots, LANES), 0)
    for half in range(2):
        own = seat[0] if half == 0 else seat[0] + 1 - 2 * (seat[0] % 2)
        start = jnp.int32(0)
        for s in range(members):
            start = start + jnp.where(s < own, vc[s], 0)
        frame = jnp.where(row < vc[own], (row + start) // FRAME_TOKENS, frames)
        first = jnp.full((vslots, LANES), LANES, jnp.int32)
        final = jnp.zeros((vslots, LANES), jnp.int32)
        for f in range(frames):
            here = frame == f
            first = jnp.where(here, ws[f], first)
            final = jnp.where(here, we[f], final)
        ok = (lane >= first) & (lane < final)
        bias[half * vslots : (half + 1) * vslots, :] = jnp.where(ok, 0.0, FAR).astype(BF)


def slabs_of(queries):
    return -(-queries // LANES)


def stat_block(st, heads, half, slots):
    rest = st.T[:heads]
    parts = []
    for _ in range(3):
        part = rest.astype(BF).astype(F32)
        parts.append(part)
        rest = rest - part
    slabs = [p[:, j * LANES : (j + 1) * LANES] for p in parts for j in range(slots)]
    slabs = slabs + [jnp.zeros_like(slabs[0])] * (8 - len(slabs))
    width = half // LANES
    groups = [
        jnp.concatenate(slabs[g : g + width], axis=1) if width > 1 else slabs[g]
        for g in range(0, 8, width)
    ]
    return jnp.concatenate(groups, axis=0).astype(BF)


def read_stats(block, heads, half, slots, turn):
    width = half // LANES
    slabs = []
    for g in range(8 // width):
        rows = block[g * heads : (g + 1) * heads]
        for j in range(width):
            slabs.append(rows[:, j * LANES : (j + 1) * LANES])
    for j in range(slots):
        total = (slabs[j] + slabs[slots + j]) + slabs[2 * slots + j]
        turn[:heads, j * LANES : (j + 1) * LANES] = total
    return turn[...].T


def chunk_features(feat, node, offset, nodes, c, aslots):
    source = lax.rem(node + offset + nodes, nodes) * 2
    own = pl.ds(pl.multiple_of((source + c) * aslots, 16), aslots)
    other = pl.ds(pl.multiple_of((source + 1 - c) * aslots, 16), aslots)
    return jnp.concatenate([feat[own, :], feat[other, :]], axis=0)


def audio_kernel(offsets, nodes, seat, feat, bias, ck, vv, ck_got, vv_got, *refs):
    count = len(offsets)
    chunks, outs, stat = refs[: 2 * count], refs[2 * count : 3 * count], refs[3 * count]
    aslots = chunks[0].shape[0]
    half = outs[0].shape[1]
    pairs = half // LANES
    c = seat[0] % 2
    node = seat[0] // 2
    masks = lane_masks()
    rows = 2 * aslots
    slots = stat.shape[0] // LANES
    lane = lax.broadcasted_iota(jnp.int32, (rows, LANES), 1)
    stat[...] = jnp.zeros_like(stat)
    stats = [jnp.zeros((rows, LANES), F32) for _ in range(count)]
    extras = [chunk_features(feat, node, o, nodes, c, aslots) for o in offsets]
    for p in range(pairs):
        cols = pl.ds(pl.multiple_of(c * half + p * LANES, LANES), LANES)
        here = slice(p * LANES, (p + 1) * LANES)
        keys = jnp.concatenate([ck[:, cols], ck_got[:, cols]], axis=0)
        keys = jnp.concatenate([keys, bias[...]], axis=1)
        values = values_of(jnp.concatenate([vv[:, cols], vv_got[:, cols]], axis=0), masks)
        for i in range(count):
            q2 = jnp.concatenate([chunks[2 * i][:, cols], chunks[2 * i + 1][:, cols]], axis=0)
            mixed, top, total = attend(q2, extras[i], keys, values, masks)
            outs[i][:rows, here] = mixed.astype(BF)
            lse = jnp.log(total)
            scaled = top * HD ** (-0.5)
            st = jnp.where(lane == 2 * p, scaled[:rows] + lse[:, :1], stats[i])
            stats[i] = jnp.where(lane == 2 * p + 1, scaled[rows:] + lse[:, HD : HD + 1], st)
    for i in range(count):
        stat[:rows, :] = stats[i]
        outs[i][rows:, :] = stat_block(stat[...], 2 * pairs, half, slots)


def video_kernel(offsets, nodes, tile, seat, feat, bias, vq, *refs):
    chunks, out = refs[: 2 * nodes], refs[2 * nodes]
    vslots, width = vq.shape
    aslots = chunks[0].shape[1]
    c = seat[0] % 2
    node = seat[0] // 2
    masks = lane_masks()
    extra = jnp.concatenate(
        [chunk_features(feat, node, o, nodes, c, aslots) for o in offsets], axis=0
    )
    for p in range(width // LANES):
        cols = slice(p * LANES, (p + 1) * LANES)
        keys = jnp.concatenate([x[0, :, cols] for x in chunks], axis=0)
        keys = jnp.concatenate([keys, extra], axis=1)
        values = values_of(jnp.concatenate([x[1, :, cols] for x in chunks], axis=0), masks)
        for t in range(vslots // tile):
            at = slice(t * tile, (t + 1) * tile)
            mixed, _, _ = attend(vq[at, cols], bias[at, :], keys, values, masks)
            out[at, cols] = mixed.astype(BF)


def self_kernel(offsets, nodes, seat, ac, feat, sq, sq_got, *refs):
    partials = refs[:nodes]
    chunks = refs[nodes : 3 * nodes]
    own_out, other_out, turn = refs[3 * nodes :]
    aslots, half = own_out.shape
    pairs = half // LANES
    heads = 2 * pairs
    slots = turn.shape[1] // LANES
    c = seat[0] % 2
    node = seat[0] // 2
    rows = 2 * aslots
    turn[...] = jnp.zeros_like(turn)
    stats = [
        read_stats(x[rows:, :].astype(F32), heads, half, slots, turn)[:rows] for x in partials
    ]
    peak = functools.reduce(jnp.maximum, stats)
    weights = [jnp.exp(s - peak) for s in stats]
    inv = 1.0 / functools.reduce(jnp.add, weights)
    weights = [w * inv for w in weights]
    masks = lane_masks()
    lane = lax.broadcasted_iota(jnp.int32, (rows, LANES), 1)
    row = lax.broadcasted_iota(jnp.int32, (rows, LANES), 0)
    mine, other = ac[seat[0]], ac[seat[0] + 1 - 2 * c]
    live = row < jnp.where(row < aslots, mine, other + aslots)
    flag = jnp.where(lane == DEAD, FAR, 0.0).astype(BF)
    extra = jnp.concatenate(
        [chunk_features(feat, node, o, nodes, c, aslots) for o in offsets], axis=0
    )
    for p in range(pairs):
        cols = pl.ds(pl.multiple_of(c * half + p * LANES, LANES), LANES)
        here = slice(p * LANES, (p + 1) * LANES)
        cross = jnp.zeros((rows, LANES), F32)
        for x, w in zip(partials, weights):
            share = jnp.where(lane < HD, w[:, 2 * p : 2 * p + 1], w[:, 2 * p + 1 : 2 * p + 2])
            cross = cross + x[:rows, here].astype(F32) * share
        q2 = jnp.concatenate([sq[:, cols], sq_got[:, cols]], axis=0)
        united = (q2.astype(F32) + cross).astype(BF)
        keys = jnp.concatenate([x[0, :, cols] for x in chunks], axis=0)
        keys = jnp.concatenate([keys, extra], axis=1)
        values = values_of(jnp.concatenate([x[1, :, cols] for x in chunks], axis=0), masks)
        mixed, _, _ = attend(united, flag, keys, values, masks)
        result = jnp.where(live, cross + mixed, 0.0).astype(BF)
        own_out[:, here] = result[:aslots]
        other_out[:, here] = result[aslots:]


def join_kernel(seat, own, got, out):
    half = own.shape[1]
    c = seat[0] % 2
    out[:, pl.ds(pl.multiple_of(c * half, LANES), half)] = own[...]
    out[:, pl.ds(pl.multiple_of((1 - c) * half, LANES), half)] = got[...]


def shards(
    video_q,
    video_cross_keys,
    video_v,
    audio_q,
    audio_k,
    audio_v,
    audio_self_q,
    audio_self_keys,
    audio_self_v,
    video_counts,
    audio_counts,
    window_start,
    window_end,
):
    seat = lax.axis_index("seq").astype(jnp.int32).reshape(1)
    members = lax.axis_size("seq")
    nodes = members // 2
    vslots, width = video_q.shape
    aslots = audio_q.shape[0]
    half = width // 2
    rows = 2 * aslots
    slots = slabs_of(rows)
    vmem = pl.BlockSpec(memory_space=pltpu.VMEM)
    smem = pl.BlockSpec(memory_space=pltpu.SMEM)

    def call(body, outs, args, scratch=(), flops=0):
        moved = sum(x.size * x.dtype.itemsize for x in args)
        return pl.pallas_call(
            body,
            out_shape=[jax.ShapeDtypeStruct(s, BF) for s in outs],
            in_specs=[smem if x.dtype == jnp.int32 else vmem for x in args],
            out_specs=[vmem] * len(outs),
            scratch_shapes=scratch,
            compiler_params=pltpu.CompilerParams(vmem_limit_bytes=20 * 2**20),
            cost_estimate=pl.CostEstimate(
                flops=flops or 1000, bytes_accessed=moved, transcendentals=0
            ),
        )(*args)

    def swap(x):
        return lax.ppermute(x, "seq", [(i, i ^ 1) for i in range(members)])

    def shift(x, by):
        pairs = [(i, (i + 2 * by) % members) for i in range(members)]
        return lax.ppermute(x, "seq", pairs)

    reach = (nodes - 1) // 2
    even = nodes % 2 == 0

    def spread(x):
        found = {0: (x, swap(x))}
        left = right = x
        for k in range(1, reach + 1):
            left = shift(left, 1)
            right = shift(right, -1)
            found[-k] = (left, swap(left))
            found[k] = (right, swap(right))
        if even:
            far = shift(left, 1)
            found[nodes // 2] = (far, swap(far))
        return found

    q_of = spread(audio_q)
    ck_got = swap(video_cross_keys)
    vv_got = swap(video_v)
    sq_got = swap(audio_self_q)
    (kv,) = call(pack_kernel, [(2, aslots, width)], (audio_k, audio_v))
    (sv,) = call(pack_kernel, [(2, aslots, width)], (audio_self_keys, audio_self_v))
    kv_of = spread(kv)
    s_of = spread(sv)
    feat, bias = call(
        functools.partial(tables_kernel, members, vslots, aslots),
        [(members * aslots, LANES), (2 * vslots, LANES)],
        (seat, video_counts, audio_counts, window_start, window_end),
    )

    unit = 4 * rows * 2 * vslots * LANES * 2

    def partial(offsets):
        chunks = [x for o in offsets for x in q_of[o]]
        return call(
            functools.partial(audio_kernel, offsets, nodes),
            [(rows + 16, half)] * len(offsets),
            (seat, feat, bias, video_cross_keys, video_v, ck_got, vv_got, *chunks),
            scratch=[pltpu.VMEM((slots * LANES, LANES), F32)],
            flops=unit * len(offsets) * (half // LANES),
        )

    parts = {}
    (parts[0],) = partial((0,))
    for k in range(1, reach + 1):
        to_left, to_right = partial((-k, k))
        parts[k] = shift(to_left, -k)
        parts[-k] = shift(to_right, k)
    if even:
        (far,) = partial((nodes // 2,))
        parts[nodes // 2] = shift(far, nodes // 2)

    offsets = tuple(sorted(q_of, key=abs))
    tile = 160 if vslots % 160 == 0 else vslots
    (video_out,) = call(
        functools.partial(video_kernel, offsets, nodes, tile),
        [(vslots, width)],
        (seat, feat, bias, video_q, *(x for o in offsets for x in kv_of[o])),
        flops=unit * nodes * (half // LANES),
    )
    own_audio, other_audio = call(
        functools.partial(self_kernel, offsets, nodes),
        [(aslots, half)] * 2,
        (
            seat,
            audio_counts,
            feat,
            audio_self_q,
            sq_got,
            *(parts[o] for o in offsets),
            *(x for o in offsets for x in s_of[o]),
        ),
        scratch=[pltpu.VMEM((LANES, slots * LANES), F32)],
        flops=unit * (half // LANES),
    )
    got_audio = swap(other_audio)
    (audio_out,) = call(join_kernel, [(aslots, width)], (seat, own_audio, got_audio))
    return (video_out, audio_out)


def solution(mesh):
    split = P(("groups", "seq"), ("heads", "sub"))

    return jax.shard_map(
        shards,
        mesh=mesh,
        in_specs=(split,) * 9 + (P("groups"),) * 4,
        out_specs=(split, split),
        check_vma=False,
    )
```
